32 devices in a mesh: batch: 2 (over x), rows: 16 (over z, y, core).
Axes of the slice: x: 2, y: 2, z: 4, core: 2. Of those that a mesh axis runs over, the one named last changes fastest.
Arguments:
- latent: bfloat16 [16, 192, 256], P(None, ('batch', 'rows')), parts along dimension 1, may hold values from -11 to 11
- kernel_in: bfloat16 [3, 3, 16, 512], replicated, may hold values from -0.5 to 0.5
- gain_one: float32 [512], replicated, may hold values from 0.25 to 1.75
- bias_one: float32 [512], replicated, may hold values from -3 to 3
- kernel_one: bfloat16 [3, 3, 512, 512], replicated, may hold values from -0.09375 to 0.09375
- gain_two: float32 [512], replicated, may hold values from 0.25 to 1.75
- bias_two: float32 [512], replicated, may hold values from -3 to 3
- kernel_two: bfloat16 [3, 3, 512, 512], replicated, may hold values from -0.09375 to 0.09375
Outputs:
- block_out: bfloat16 [192, 256, 512], P(('batch', 'rows')), parts along dimension 0
The draws below stay inside these ranges and needn't reach their ends.
There are 2 independent parts, one for each index of `batch`. The reference program is written for one: setup_inputs(seed, part) draws one part's arguments, and reference() takes and returns one part's arrays. A program takes and returns all parts, laid end to end along the dimension named above; an argument that names none is the same for every part. Nothing has to cross between parts.
All inputs are finite; a program needn't handle non-finite values.
Results may differ from the reference program's by a relative error of at most 0.014.
Values may be sent and summed in bfloat16 or wider, within the bound.
A program may use at most 64 MiB of HBM per device.

```python
import jax
import jax.numpy as jnp
from jax import lax

C = 512
GROUPS = 32
LC = 16
COLS = 256
HEIGHT = 96


def draw_latent(key, part):
    keys = jax.random.split(jax.random.fold_in(key, 11), 7)
    heights = jnp.arange(HEIGHT, dtype=jnp.float32) / (HEIGHT - 1)
    direction = (2 * jax.random.randint(keys[0], (), 0, 2) - 1).astype(jnp.float32)
    trend = direction * 0.9 * (2.0 * heights - 1.0)
    rough = jax.random.uniform(keys[1], (HEIGHT,), jnp.float32, -0.3, 0.3)
    switch = jax.random.uniform(keys[2], (), jnp.float32, 0.3, 0.7)
    side = jnp.where(heights < switch, -1.0, 1.0)
    level = jax.random.uniform(keys[3], (LC, 1, 1), jnp.float32, -0.3, 0.3)
    offset = level * side[None, :, None] + jax.random.uniform(keys[4], (LC, HEIGHT, 1), jnp.float32, -0.1, 0.1)
    row_ids = jnp.arange(HEIGHT, dtype=jnp.int32)
    col_ids = jnp.arange(COLS, dtype=jnp.int32)
    row_edge = (row_ids == 0) | (row_ids == HEIGHT - 1)
    col_edge = (col_ids == 0) | (col_ids == COLS - 1)
    border = row_edge[:, None] | col_edge[None, :]
    inner_scale = 0.2 * jnp.exp(trend + rough)
    outer_scale = 4.5 * jnp.exp(0.5 * trend + rough)
    outer_noise = jax.random.uniform(keys[6], (LC, HEIGHT, COLS), jnp.float32, -1.0, 1.0)
    noise = jnp.clip(jax.random.normal(keys[5], (LC, HEIGHT, COLS), jnp.float32), -4.0, 4.0)
    inner = noise * inner_scale[None, :, None]
    outer = outer_noise * outer_scale[None, :, None]
    values = offset + jnp.where(border[None, :, :], outer, inner)
    return values.astype(jnp.bfloat16)


def normal_values(own_key, dims, scale, limit, held_as=jnp.bfloat16):
    return jnp.clip(scale * jax.random.normal(own_key, dims, jnp.float32), -limit, limit).astype(held_as)


def setup_inputs(seed: int = 0, part: int = 0) -> dict:
    streams_of = jax.random.split(jax.random.key(seed), 9)
    own_keys = jax.random.split(jax.random.fold_in(streams_of[8], part), 9)
    return {
        "latent": draw_latent(jax.random.fold_in(jax.random.fold_in(streams_of[8], part), 71), part),
        "kernel_in": normal_values(streams_of[1], (3, 3, LC, C), (9 * LC) ** -0.5, 0.5),
        "gain_one": jnp.clip(1.0 + 0.15 * jax.random.normal(streams_of[2], (C,), jnp.float32), 0.25, 1.75),
        "bias_one": normal_values(streams_of[3], (C,), 0.5, 3.0, jnp.float32),
        "kernel_one": normal_values(streams_of[4], (3, 3, C, C), (9 * C) ** -0.5, 0.09375),
        "gain_two": jnp.clip(1.0 + 0.15 * jax.random.normal(streams_of[5], (C,), jnp.float32), 0.25, 1.75),
        "bias_two": normal_values(streams_of[6], (C,), 0.5, 3.0, jnp.float32),
        "kernel_two": normal_values(streams_of[7], (3, 3, C, C), (9 * C) ** -0.5, 0.09375),
    }


EPSILON = 1e-06

def convolve(padded, kernel):
    height = padded.shape[0] - 2
    width = padded.shape[1] - 2
    inputs = padded.shape[2]
    total = jnp.zeros((height * width, kernel.shape[3]), jnp.float32)
    for row_shift in range(3):
        band = padded[row_shift:row_shift + height]
        stacked = jnp.concatenate([band[:, col_shift:col_shift + width] for col_shift in range(3)], axis=-1)
        total = total + jnp.dot(stacked.reshape(height * width, 3 * inputs).astype(jnp.float32), kernel[row_shift].reshape(3 * inputs, -1).astype(jnp.float32), preferred_element_type=jnp.float32)
    return total.reshape(height, width, -1)

def pad_cells(field):
    return jnp.pad(field, ((1, 1), (1, 1), (0, 0)))

def group_activate(field, gain, bias):
    values = field.astype(jnp.float32).reshape(field.shape[0], field.shape[1], GROUPS, -1)
    center = lax.optimization_barrier(jnp.mean(values, axis=(0, 1, 3)))
    spread = lax.optimization_barrier(jnp.mean((values - center[None, None, :, None]) ** 2, axis=(0, 1, 3)))
    normed = (values - center[None, None, :, None]) * lax.rsqrt(spread + EPSILON)[None, None, :, None]
    normed = normed.reshape(field.shape) * gain + bias
    return jax.nn.silu(normed).astype(jnp.bfloat16)

def reference(latent, kernel_in, gain_one, bias_one, kernel_one, gain_two, bias_two, kernel_two):
    image = jnp.transpose(latent, (1, 2, 0))
    features = convolve(pad_cells(image), kernel_in).astype(jnp.bfloat16)
    first = group_activate(features, gain_one, bias_one)
    hidden = convolve(pad_cells(first), kernel_one).astype(jnp.bfloat16)
    second = group_activate(hidden, gain_two, bias_two)
    result = features.astype(jnp.float32) + convolve(pad_cells(second), kernel_two)
    return result.astype(jnp.bfloat16)
```

```python
import functools

import jax
import jax.numpy as jnp
from jax import lax
from jax.experimental import pallas as pl
from jax.experimental.pallas import tpu as pltpu
from jax.sharding import PartitionSpec as P

GROUPS = 32
EPSILON = 1e-06
MESH = pl.DeviceIdType.MESH


def lane_group_sum(values, width):
    lanes = values.shape[1]
    index = lax.broadcasted_iota(jnp.int32, values.shape, 1)
    step = 1
    while step < width:
        up = pltpu.roll(values, step, 1)
        down = pltpu.roll(values, lanes - step, 1)
        values = values + jnp.where((index // step) % 2 == 1, up, down)
        step *= 2
    return values


def shifted(values, amount):
    count = values.shape[0]
    index = lax.broadcasted_iota(jnp.int32, values.shape, 0)
    if amount == 1:
        return jnp.where(index == 0, 0.0, pltpu.roll(values, 1, 0))
    return jnp.where(index == count - 1, 0.0, pltpu.roll(values, count - 1, 0))


def kernel(
    n,
    block,
    latent_ref,
    kin_ref,
    gain_one_ref,
    bias_one_ref,
    gain_two_ref,
    bias_two_ref,
    k1_hbm,
    k2_hbm,
    out_hbm,
    k1,
    k2,
    lat,
    feat,
    stack,
    hid,
    result,
    stat_one,
    stat_two,
    acc,
    weight_sem,
    out_sem,
    lat_send,
    lat_recv,
    hid_send,
    hid_recv,
    one_send,
    one_recv,
    two_send,
    two_recv,
):
    me = lax.axis_index("rows")
    height, channels_in, width = latent_ref.shape
    features = feat.shape[2]
    blocks = height // block
    has_up = me > 0
    has_down = me < n - 1
    up = lax.rem(me + n - 1, n)
    down = lax.rem(me + 1, n)

    barrier = pltpu.get_barrier_semaphore()

    def greet(d, carry):
        pl.semaphore_signal(
            barrier, inc=1, device_id={"rows": lax.rem(me + d, n)}, device_id_type=MESH
        )
        return carry

    lax.fori_loop(1, n, greet, 0)
    fetch_one = pltpu.make_async_copy(k1_hbm, k1, weight_sem.at[0])
    fetch_two = pltpu.make_async_copy(k2_hbm, k2, weight_sem.at[1])
    fetch_one.start()

    def remote(src, dst, send, recv, target):
        return pltpu.make_async_remote_copy(
            src_ref=src,
            dst_ref=dst,
            send_sem=send,
            recv_sem=recv,
            device_id={"rows": target},
            device_id_type=MESH,
        )

    lat[pl.ds(2, height)] = latent_ref[...]

    @pl.when(jnp.logical_not(has_up))
    def _():
        lat[pl.ds(0, 2)] = jnp.zeros((2, channels_in, width), lat.dtype)
        hid[pl.ds(0, 1)] = jnp.zeros((1, width, features), hid.dtype)

    @pl.when(jnp.logical_not(has_down))
    def _():
        lat[pl.ds(height + 2, 2)] = jnp.zeros((2, channels_in, width), lat.dtype)
        hid[pl.ds(height + 1, 1)] = jnp.zeros((1, width, features), hid.dtype)

    column = lax.broadcasted_iota(jnp.int32, (channels_in, width), 1)

    def feature_row(index, count):
        pieces = []
        for a in range(3):
            row = lat[index + a].astype(jnp.float32)
            left = jnp.where(column == 0, 0.0, pltpu.roll(row, 1, 1))
            right = jnp.where(column == width - 1, 0.0, pltpu.roll(row, width - 1, 1))
            for piece in (left, row, right):
                pieces.append(piece.astype(jnp.bfloat16))
        taps = jnp.concatenate(pieces, axis=0)
        row = lax.dot_general(
            taps,
            kin_ref[...],
            (((0,), (0,)), ((), ())),
            preferred_element_type=jnp.float32,
        ).astype(jnp.bfloat16)
        feat[index] = row
        if count:
            add_moments(row)

    def add_moments(row):
        values = row.astype(jnp.float32).reshape(-1, 8, features)
        acc[0] += jnp.sum(values, axis=0)
        acc[1] += jnp.sum(values * values, axis=0)

    def clear_moments():
        acc[...] = jnp.zeros_like(acc)

    def publish(stat, send, recv):
        stat[0] = jnp.sum(acc[...], axis=1)

        def body(d, carry):
            remote(
                stat.at[0], stat.at[d], send.at[d], recv.at[d], lax.rem(me + d, n)
            ).start()
            return carry

        lax.fori_loop(1, n, body, 0)

    def collect(stat, send, recv, gain_ref, bias_ref):
        def body(d, carry):
            remote(
                stat.at[0], stat.at[d], send.at[d], recv.at[d], lax.rem(me + d, n)
            ).wait()
            return carry

        lax.fori_loop(1, n, body, 0)
        totals = jnp.sum(stat[...], axis=0)
        per_group = features // GROUPS
        totals = lane_group_sum(totals, per_group)
        moments = totals / (n * height * width * per_group)
        center = moments[0:1]
        spread = jnp.maximum(moments[1:2] - center * center, 0.0)
        scale = lax.rsqrt(spread + EPSILON) * gain_ref[...]
        return scale, bias_ref[...] - center * scale

    def activate_row(source, index, scale, offset, edge):
        values = source[index].astype(jnp.float32)
        half = (values * scale + offset) * 0.5
        values = half + half * jnp.tanh(half)
        if edge is not None:
            values = jnp.where(edge, values, 0.0)
        stack[index, :, pl.ds(features, features)] = values.astype(jnp.bfloat16)
        stack[index, :, pl.ds(0, features)] = shifted(values, 1).astype(jnp.bfloat16)
        stack[index, :, pl.ds(2 * features, features)] = shifted(values, -1).astype(
            jnp.bfloat16
        )

    def convolve_rows(start, weights):
        total = None
        for a in range(3):
            lhs = stack[pl.ds(start + a, block)].reshape(block * width, 3 * features)
            part = jnp.dot(lhs, weights[a], preferred_element_type=jnp.float32)
            total = part if total is None else total + part
        return total

    lat_up = remote(
        latent_ref.at[pl.ds(0, 2)],
        lat.at[pl.ds(height + 2, 2)],
        lat_send.at[0],
        lat_recv.at[0],
        up,
    )
    lat_down = remote(
        latent_ref.at[pl.ds(height - 2, 2)],
        lat.at[pl.ds(0, 2)],
        lat_send.at[1],
        lat_recv.at[1],
        down,
    )
    pl.semaphore_wait(barrier, n - 1)

    @pl.when(has_up)
    def _():
        lat_up.start()

    @pl.when(has_down)
    def _():
        lat_down.start()

    clear_moments()

    def inner(index, carry):
        feature_row(index, True)
        return carry

    lax.fori_loop(2, height, inner, 0)

    @pl.when(has_up)
    def _():
        lat_up.wait_send()
        lat_down.wait_recv()

    @pl.when(has_down)
    def _():
        lat_down.wait_send()
        lat_up.wait_recv()

    def edge_row(k, carry):
        feature_row(1 + k * (height - 1), True)
        return carry

    lax.fori_loop(0, 2, edge_row, 0)
    publish(stat_one, one_send, one_recv)
    fetch_two.start()

    def halo_row(k, carry):
        feature_row(k * (height + 1), False)
        return carry

    lax.fori_loop(0, 2, halo_row, 0)
    clear_moments()
    scale, offset = collect(stat_one, one_send, one_recv, gain_one_ref, bias_one_ref)

    def first_row(index, carry):
        inside = jnp.logical_and(
            jnp.logical_or(has_up, index > 0), jnp.logical_or(has_down, index < height + 1)
        )
        activate_row(feat, index, scale, offset, inside)
        return carry

    lax.fori_loop(0, height + 2, first_row, 0)
    fetch_one.wait()

    hid_up = remote(hid.at[1], hid.at[height + 1], hid_send.at[0], hid_recv.at[0], up)
    hid_down = remote(hid.at[height], hid.at[0], hid_send.at[1], hid_recv.at[1], down)

    def hidden_block(step, carry):
        start = lax.rem(step + blocks - 1, blocks) * block
        rows = convolve_rows(start, k1).astype(jnp.bfloat16)
        hid[pl.ds(start + 1, block)] = rows.reshape(block, width, features)
        add_moments(rows)

        @pl.when(jnp.logical_and(start == 0, has_up))
        def _():
            hid_up.start()

        @pl.when(jnp.logical_and(start == height - block, has_down))
        def _():
            hid_down.start()

        return carry

    lax.fori_loop(0, blocks, hidden_block, 0)
    publish(stat_two, two_send, two_recv)
    scale, offset = collect(stat_two, two_send, two_recv, gain_two_ref, bias_two_ref)

    def second_row(index, carry):
        activate_row(hid, index, scale, offset, None)
        return carry

    lax.fori_loop(1, height + 1, second_row, 0)

    @pl.when(has_up)
    def _():
        hid_up.wait_send()
        hid_down.wait_recv()

    @pl.when(has_down)
    def _():
        hid_down.wait_send()
        hid_up.wait_recv()

    def second_edge(k, carry):
        inside = jnp.logical_or(
            jnp.logical_and(has_up, k == 0), jnp.logical_and(has_down, k == 1)
        )
        activate_row(hid, k * (height + 1), scale, offset, inside)
        return carry

    lax.fori_loop(0, 2, second_edge, 0)
    fetch_two.wait()

    def store(step):
        return pltpu.make_async_copy(
            result.at[pl.ds(step * block, block)],
            out_hbm.at[pl.ds(step * block, block)],
            out_sem.at[step],
        )

    def final_block(step, carry):
        start = step * block
        rows = convolve_rows(start, k2).reshape(block, width, features)
        rows = rows + feat[pl.ds(start + 1, block)].astype(jnp.float32)
        result[pl.ds(start, block)] = rows.astype(jnp.bfloat16)
        store(step).start()
        return carry

    lax.fori_loop(0, blocks, final_block, 0)

    def drain(step, carry):
        store(step).wait()
        return carry

    lax.fori_loop(0, blocks, drain, 0)


def local(n, latent, kernel_in, gain_one, bias_one, kernel_one, gain_two, bias_two, kernel_two):
    channels_in, height, width = latent.shape
    features = kernel_in.shape[3]
    block = 2 if height % 2 == 0 else 1
    bf16 = jnp.bfloat16
    vmem = pl.BlockSpec(memory_space=pltpu.VMEM)
    hbm = pl.BlockSpec(memory_space=pl.ANY)
    dma = pltpu.SemaphoreType.DMA
    return pl.pallas_call(
        functools.partial(kernel, n, block),
        out_shape=jax.ShapeDtypeStruct((height, width, features), bf16),
        in_specs=[vmem] * 6 + [hbm] * 2,
        out_specs=hbm,
        scratch_shapes=[
            pltpu.VMEM((3, 3 * features, features), bf16),
            pltpu.VMEM((3, 3 * features, features), bf16),
            pltpu.VMEM((height + 4, channels_in, width), bf16),
            pltpu.VMEM((height + 2, width, features), bf16),
            pltpu.VMEM((height + 2, width, 3 * features), bf16),
            pltpu.VMEM((height + 2, width, features), bf16),
            pltpu.VMEM((height, width, features), bf16),
            pltpu.VMEM((n, 2, features), jnp.float32),
            pltpu.VMEM((n, 2, features), jnp.float32),
            pltpu.VMEM((2, 8, features), jnp.float32),
            dma((2,)),
            dma((height // block,)),
            dma((2,)),
            dma((2,)),
            dma((2,)),
            dma((2,)),
            dma((n,)),
            dma((n,)),
            dma((n,)),
            dma((n,)),
        ],
        compiler_params=pltpu.CompilerParams(
            collective_id=0, has_side_effects=True, vmem_limit_bytes=56 * 1024 * 1024
        ),
        name="resblock",
    )(
        jnp.transpose(latent, (1, 0, 2)),
        kernel_in.reshape(9 * channels_in, features),
        gain_one.reshape(1, -1),
        bias_one.reshape(1, -1),
        gain_two.reshape(1, -1),
        bias_two.reshape(1, -1),
        kernel_one.reshape(3, 3 * features, features),
        kernel_two.reshape(3, 3 * features, features),
    )


def solution(mesh):
    in_specs = (P(None, ("batch", "rows"), None), P(), P(), P(), P(), P(), P(), P())
    out_specs = P(("batch", "rows"), None, None)
    return jax.shard_map(
        functools.partial(local, mesh.shape["rows"]),
        mesh=mesh,
        in_specs=in_specs,
        out_specs=out_specs,
        check_vma=False,
    )
```

```python
import functools

import jax
import jax.numpy as jnp
from jax import lax
from jax.experimental import pallas as pl
from jax.experimental.pallas import tpu as pltpu
from jax.sharding import PartitionSpec as P

GROUPS = 32
EPSILON = 1e-06
MESH = pl.DeviceIdType.MESH


def lane_group_sum(values, width):
    lanes = values.shape[1]
    index = lax.broadcasted_iota(jnp.int32, values.shape, 1)
    step = 1
    while step < width:
        up = pltpu.roll(values, step, 1)
        down = pltpu.roll(values, lanes - step, 1)
        values = values + jnp.where((index // step) % 2 == 1, up, down)
        step *= 2
    return values


def packed(sums):
    features = sums.shape[1]
    per_group = features // GROUPS
    chunks = features // 128
    sums = lane_group_sum(sums, per_group)
    slot = lax.broadcasted_iota(jnp.int32, (1, 128), 1) % per_group
    row = jnp.zeros((1, 128), jnp.float32)
    for q in range(2):
        for j in range(chunks):
            row = jnp.where(
                slot == q * chunks + j, sums[q : q + 1, 128 * j : 128 * j + 128], row
            )
    return row


def unpacked(row, features):
    per_group = features // GROUPS
    chunks = features // 128
    shape = (2 * chunks, 128)
    slot = lax.broadcasted_iota(jnp.int32, shape, 1) % per_group
    wanted = lax.broadcasted_iota(jnp.int32, shape, 0)
    rows = jnp.where(slot == wanted, jnp.broadcast_to(row, shape), 0.0)
    rows = lane_group_sum(rows, per_group)
    return [
        jnp.concatenate(
            [rows[q * chunks + j : q * chunks + j + 1] for j in range(chunks)], axis=1
        )
        for q in range(2)
    ]


def shifted(values, amount):
    count = values.shape[0]
    index = lax.broadcasted_iota(jnp.int32, values.shape, 0)
    if amount == 1:
        return jnp.where(index == 0, 0.0, pltpu.roll(values, 1, 0))
    return jnp.where(index == count - 1, 0.0, pltpu.roll(values, count - 1, 0))


def kernel(
    n,
    block,
    latent_hbm,
    kin_hbm,
    gain_one_hbm,
    bias_one_hbm,
    gain_two_hbm,
    bias_two_hbm,
    k1_hbm,
    k2_hbm,
    result,
    kin_ref,
    gain_one_ref,
    bias_one_ref,
    gain_two_ref,
    bias_two_ref,
    k1,
    k2,
    lat,
    feat,
    stack,
    hid,
    stat_one,
    stat_two,
    acc,
    weight_sem,
    small_sem,
    lat_send,
    lat_recv,
    hid_send,
    hid_recv,
    one_send,
    one_recv,
    two_send,
    two_recv,
):
    me = lax.axis_index("rows")
    height, channels_in, width = latent_hbm.shape
    features = feat.shape[2]
    blocks = height // block
    has_up = me > 0
    has_down = me < n - 1
    up = lax.rem(me + n - 1, n)
    down = lax.rem(me + 1, n)

    barrier = pltpu.get_barrier_semaphore()

    def greet(d, carry):
        pl.semaphore_signal(
            barrier, inc=1, device_id={"rows": lax.rem(me + d, n)}, device_id_type=MESH
        )
        return carry

    lax.fori_loop(1, n, greet, 0)
    fetch_one = pltpu.make_async_copy(k1_hbm, k1, weight_sem.at[0])
    fetch_two = pltpu.make_async_copy(k2_hbm, k2, weight_sem.at[1])
    small = [
        pltpu.make_async_copy(src, dst, small_sem.at[i])
        for i, (src, dst) in enumerate(
            (
                (latent_hbm, lat.at[pl.ds(2, height)]),
                (kin_hbm, kin_ref),
                (gain_one_hbm, gain_one_ref),
                (bias_one_hbm, bias_one_ref),
                (gain_two_hbm, gain_two_ref),
                (bias_two_hbm, bias_two_ref),
            )
        )
    ]
    for copy in small:
        copy.start()
    fetch_one.start()

    def remote(src, dst, send, recv, target):
        return pltpu.make_async_remote_copy(
            src_ref=src,
            dst_ref=dst,
            send_sem=send,
            recv_sem=recv,
            device_id={"rows": target},
            device_id_type=MESH,
        )

    @pl.when(jnp.logical_not(has_up))
    def _():
        lat[pl.ds(0, 2)] = jnp.zeros((2, channels_in, width), lat.dtype)
        hid[pl.ds(0, 1)] = jnp.zeros((1, width, features), hid.dtype)

    @pl.when(jnp.logical_not(has_down))
    def _():
        lat[pl.ds(height + 2, 2)] = jnp.zeros((2, channels_in, width), lat.dtype)
        hid[pl.ds(height + 1, 1)] = jnp.zeros((1, width, features), hid.dtype)

    column = lax.broadcasted_iota(jnp.int32, (channels_in, width), 1)

    def feature_row(index, count):
        pieces = []
        for a in range(3):
            row = lat[index + a].astype(jnp.float32)
            left = jnp.where(column == 0, 0.0, pltpu.roll(row, 1, 1))
            right = jnp.where(column == width - 1, 0.0, pltpu.roll(row, width - 1, 1))
            for piece in (left, row, right):
                pieces.append(piece.astype(jnp.bfloat16))
        taps = jnp.concatenate(pieces, axis=0)
        row = lax.dot_general(
            taps,
            kin_ref[...],
            (((0,), (0,)), ((), ())),
            preferred_element_type=jnp.float32,
        ).astype(jnp.bfloat16)
        feat[index] = row
        if count:
            add_moments(row)

    def add_moments(row):
        values = row.astype(jnp.float32).reshape(-1, 8, features)
        acc[0] += jnp.sum(values, axis=0)
        acc[1] += jnp.sum(values * values, axis=0)

    def clear_moments():
        acc[...] = jnp.zeros_like(acc)

    def publish(stat, send, recv):
        stat[0] = packed(jnp.sum(acc[...], axis=1))

        def body(d, carry):
            remote(
                stat.at[0], stat.at[d], send.at[d], recv.at[d], lax.rem(me + d, n)
            ).start()
            return carry

        lax.fori_loop(1, n, body, 0)

    def collect(stat, send, recv, gain_ref, bias_ref):
        def body(d, carry):
            remote(
                stat.at[0], stat.at[d], send.at[d], recv.at[d], lax.rem(me + d, n)
            ).wait()
            return carry

        lax.fori_loop(1, n, body, 0)
        row = jnp.sum(stat[...].reshape(n, 128), axis=0, keepdims=True)
        count = n * height * width * (features // GROUPS)
        center, square = [total / count for total in unpacked(row, features)]
        spread = jnp.maximum(square - center * center, 0.0)
        scale = lax.rsqrt(spread + EPSILON) * gain_ref[...]
        return scale, bias_ref[...] - center * scale

    def activate_row(source, index, scale, offset, edge):
        values = source[index].astype(jnp.float32)
        half = (values * scale + offset) * 0.5
        values = half + half * jnp.tanh(half)
        if edge is not None:
            values = jnp.where(edge, values, 0.0)
        stack[index, :, pl.ds(features, features)] = values.astype(jnp.bfloat16)
        stack[index, :, pl.ds(0, features)] = shifted(values, 1).astype(jnp.bfloat16)
        stack[index, :, pl.ds(2 * features, features)] = shifted(values, -1).astype(
            jnp.bfloat16
        )

    def convolve_rows(start, weights):
        total = None
        for a in range(3):
            lhs = stack[pl.ds(start + a, block)].reshape(block * width, 3 * features)
            part = jnp.dot(lhs, weights[a], preferred_element_type=jnp.float32)
            total = part if total is None else total + part
        return total

    lat_up = remote(
        lat.at[pl.ds(2, 2)],
        lat.at[pl.ds(height + 2, 2)],
        lat_send.at[0],
        lat_recv.at[0],
        up,
    )
    lat_down = remote(
        lat.at[pl.ds(height, 2)],
        lat.at[pl.ds(0, 2)],
        lat_send.at[1],
        lat_recv.at[1],
        down,
    )
    for copy in small:
        copy.wait()
    pl.semaphore_wait(barrier, n - 1)

    @pl.when(has_up)
    def _():
        lat_up.start()

    @pl.when(has_down)
    def _():
        lat_down.start()

    clear_moments()

    def inner(index, carry):
        feature_row(index, True)
        return carry

    lax.fori_loop(2, height, inner, 0)

    @pl.when(has_up)
    def _():
        lat_up.wait_send()
        lat_down.wait_recv()

    @pl.when(has_down)
    def _():
        lat_down.wait_send()
        lat_up.wait_recv()

    def edge_row(k, carry):
        feature_row(1 + k * (height - 1), True)
        return carry

    lax.fori_loop(0, 2, edge_row, 0)
    publish(stat_one, one_send, one_recv)
    fetch_two.start()

    def halo_row(k, carry):
        feature_row(k * (height + 1), False)
        return carry

    lax.fori_loop(0, 2, halo_row, 0)
    clear_moments()
    scale, offset = collect(stat_one, one_send, one_recv, gain_one_ref, bias_one_ref)

    def inside(index):
        if index == 0:
            return has_up
        if index == height + 1:
            return has_down
        return None

    def rows_of(number):
        return range(number * block, number * block + block + 2)

    def run_blocks(source, order, scale, offset, before_halo, ready, emit):
        done = set()
        halo_ready = False

        def fill(indices):
            nonlocal halo_ready
            for index in indices:
                if index in done:
                    continue
                if inside(index) is not None and not halo_ready:
                    before_halo()
                    halo_ready = True
                done.add(index)
                activate_row(source, index, scale, offset, inside(index))

        fill(rows_of(order[0]))
        ready()
        for step, number in enumerate(order):
            following = rows_of(order[step + 1]) if step + 1 < len(order) else ()
            new = [index for index in following if index not in done]
            if not halo_ready and any(inside(index) is not None for index in new):
                before_halo()
                halo_ready = True
            emit(number, lambda: fill(new))

    hid_up = remote(hid.at[1], hid.at[height + 1], hid_send.at[0], hid_recv.at[0], up)
    hid_down = remote(hid.at[height], hid.at[0], hid_send.at[1], hid_recv.at[1], down)

    def hidden_block(number, beside):
        start = number * block
        rows = convolve_rows(start, k1).astype(jnp.bfloat16)
        beside()
        hid[pl.ds(start + 1, block)] = rows.reshape(block, width, features)
        add_moments(rows)
        if start == 0:

            @pl.when(has_up)
            def _():
                hid_up.start()

        if start == height - block:

            @pl.when(has_down)
            def _():
                hid_down.start()

    last = blocks - 1
    run_blocks(
        feat,
        [last] + list(range(last)),
        scale,
        offset,
        lambda: None,
        fetch_one.wait,
        hidden_block,
    )
    publish(stat_two, two_send, two_recv)
    scale, offset = collect(stat_two, two_send, two_recv, gain_two_ref, bias_two_ref)

    def wait_hidden():
        @pl.when(has_up)
        def _():
            hid_up.wait_send()
            hid_down.wait_recv()

        @pl.when(has_down)
        def _():
            hid_down.wait_send()
            hid_up.wait_recv()

    def final_block(number, beside):
        start = number * block
        rows = convolve_rows(start, k2).reshape(block, width, features)
        beside()
        rows = rows + feat[pl.ds(start + 1, block)].astype(jnp.float32)
        result[pl.ds(start, block)] = rows.astype(jnp.bfloat16)

    run_blocks(
        hid,
        list(range(1, blocks)) + [0],
        scale,
        offset,
        wait_hidden,
        fetch_two.wait,
        final_block,
    )


def local(n, latent, kernel_in, gain_one, bias_one, kernel_one, gain_two, bias_two, kernel_two):
    channels_in, height, width = latent.shape
    features = kernel_in.shape[3]
    block = 2 if height % 2 == 0 else 1
    bf16 = jnp.bfloat16
    vmem = pl.BlockSpec(memory_space=pltpu.VMEM)
    hbm = pl.BlockSpec(memory_space=pl.ANY)
    dma = pltpu.SemaphoreType.DMA
    return pl.pallas_call(
        functools.partial(kernel, n, block),
        out_shape=pltpu.VMEM((height, width, features), bf16),
        in_specs=[hbm] * 8,
        out_specs=vmem,
        scratch_shapes=[
            pltpu.VMEM((9 * channels_in, features), bf16),
            pltpu.VMEM((1, features), jnp.float32),
            pltpu.VMEM((1, features), jnp.float32),
            pltpu.VMEM((1, features), jnp.float32),
            pltpu.VMEM((1, features), jnp.float32),
            pltpu.VMEM((3, 3 * features, features), bf16),
            pltpu.VMEM((3, 3 * features, features), bf16),
            pltpu.VMEM((height + 4, channels_in, width), bf16),
            pltpu.VMEM((height + 2, width, features), bf16),
            pltpu.VMEM((height + 2, width, 3 * features), bf16),
            pltpu.VMEM((height + 2, width, features), bf16),
            pltpu.VMEM((n, 1, 128), jnp.float32),
            pltpu.VMEM((n, 1, 128), jnp.float32),
            pltpu.VMEM((2, 8, features), jnp.float32),
            dma((2,)),
            dma((6,)),
            dma((2,)),
            dma((2,)),
            dma((2,)),
            dma((2,)),
            dma((n,)),
            dma((n,)),
            dma((n,)),
            dma((n,)),
        ],
        compiler_params=pltpu.CompilerParams(
            collective_id=0, has_side_effects=True, vmem_limit_bytes=56 * 1024 * 1024
        ),
        name="resblock",
    )(
        jnp.transpose(latent, (1, 0, 2)),
        kernel_in.reshape(9 * channels_in, features),
        gain_one.reshape(1, -1),
        bias_one.reshape(1, -1),
        gain_two.reshape(1, -1),
        bias_two.reshape(1, -1),
        kernel_one.reshape(3, 3 * features, features),
        kernel_two.reshape(3, 3 * features, features),
    )


def solution(mesh):
    in_specs = (P(None, ("batch", "rows"), None), P(), P(), P(), P(), P(), P(), P())
    out_specs = P(("batch", "rows"), None, None)
    return jax.shard_map(
        functools.partial(local, mesh.shape["rows"]),
        mesh=mesh,
        in_specs=in_specs,
        out_specs=out_specs,
        check_vma=False,
    )
```

```python
import functools

import jax
import jax.numpy as jnp
from jax import lax
from jax.experimental import pallas as pl
from jax.experimental.pallas import tpu as pltpu
from jax.sharding import PartitionSpec as P

GROUPS = 32
EPSILON = 1e-06
MESH = pl.DeviceIdType.MESH


def lane_group_sum(values, width):
    lanes = values.shape[1]
    index = lax.broadcasted_iota(jnp.int32, values.shape, 1)
    step = 1
    while step < width:
        up = pltpu.roll(values, step, 1)
        down = pltpu.roll(values, lanes - step, 1)
        values = values + jnp.where((index // step) % 2 == 1, up, down)
        step *= 2
    return values


def packed(sums):
    features = sums.shape[1]
    per_group = features // GROUPS
    chunks = features // 128
    sums = lane_group_sum(sums, per_group)
    slot = lax.broadcasted_iota(jnp.int32, (1, 128), 1) % per_group
    row = jnp.zeros((1, 128), jnp.float32)
    for q in range(2):
        for j in range(chunks):
            row = jnp.where(
                slot == q * chunks + j, sums[q : q + 1, 128 * j : 128 * j + 128], row
            )
    return row


def unpacked(row, features):
    per_group = features // GROUPS
    chunks = features // 128
    shape = (2 * chunks, 128)
    slot = lax.broadcasted_iota(jnp.int32, shape, 1) % per_group
    wanted = lax.broadcasted_iota(jnp.int32, shape, 0)
    rows = jnp.where(slot == wanted, jnp.broadcast_to(row, shape), 0.0)
    rows = lane_group_sum(rows, per_group)
    return [
        jnp.concatenate(
            [rows[q * chunks + j : q * chunks + j + 1] for j in range(chunks)], axis=1
        )
        for q in range(2)
    ]


def shifted(values, amount):
    count = values.shape[0]
    index = lax.broadcasted_iota(jnp.int32, values.shape, 0)
    if amount == 1:
        return jnp.where(index == 0, 0.0, pltpu.roll(values, 1, 0))
    return jnp.where(index == count - 1, 0.0, pltpu.roll(values, count - 1, 0))


def kernel(
    n,
    block,
    latent_hbm,
    kin_hbm,
    gain_one_hbm,
    bias_one_hbm,
    gain_two_hbm,
    bias_two_hbm,
    k1_hbm,
    k2_hbm,
    result,
    kin_ref,
    gain_one_ref,
    bias_one_ref,
    gain_two_ref,
    bias_two_ref,
    k1,
    k2,
    lat,
    feat,
    stack,
    hid,
    stat_one,
    stat_two,
    acc,
    weight_sem,
    small_sem,
    lat_send,
    lat_recv,
    hid_send,
    hid_recv,
    one_send,
    one_recv,
    two_send,
    two_recv,
):
    me = lax.axis_index("rows")
    height, channels_in, width = latent_hbm.shape
    features = feat.shape[2]
    blocks = height // block
    has_up = me > 0
    has_down = me < n - 1
    up = lax.rem(me + n - 1, n)
    down = lax.rem(me + 1, n)

    barrier = pltpu.get_barrier_semaphore()

    def greet(d, carry):
        pl.semaphore_signal(
            barrier, inc=1, device_id={"rows": lax.rem(me + d, n)}, device_id_type=MESH
        )
        return carry

    lax.fori_loop(1, n, greet, 0)
    fetch_one = pltpu.make_async_copy(k1_hbm, k1, weight_sem.at[0])
    fetch_two = pltpu.make_async_copy(k2_hbm, k2, weight_sem.at[1])
    small = [
        pltpu.make_async_copy(src, dst, small_sem.at[i])
        for i, (src, dst) in enumerate(
            (
                (latent_hbm, lat.at[pl.ds(2, height)]),
                (kin_hbm, kin_ref),
                (gain_one_hbm, gain_one_ref),
                (bias_one_hbm, bias_one_ref),
                (gain_two_hbm, gain_two_ref),
                (bias_two_hbm, bias_two_ref),
            )
        )
    ]
    for copy in small:
        copy.start()
    fetch_one.start()

    def remote(src, dst, send, recv, target):
        return pltpu.make_async_remote_copy(
            src_ref=src,
            dst_ref=dst,
            send_sem=send,
            recv_sem=recv,
            device_id={"rows": target},
            device_id_type=MESH,
        )

    @pl.when(jnp.logical_not(has_up))
    def _():
        lat[pl.ds(0, 2)] = jnp.zeros((2, channels_in, width), lat.dtype)
        hid[pl.ds(0, 1)] = jnp.zeros((1, width, features), hid.dtype)

    @pl.when(jnp.logical_not(has_down))
    def _():
        lat[pl.ds(height + 2, 2)] = jnp.zeros((2, channels_in, width), lat.dtype)
        hid[pl.ds(height + 1, 1)] = jnp.zeros((1, width, features), hid.dtype)

    column = lax.broadcasted_iota(jnp.int32, (channels_in, width), 1)

    def feature_row(index, count):
        pieces = []
        for a in range(3):
            row = lat[index + a].astype(jnp.float32)
            left = jnp.where(column == 0, 0.0, pltpu.roll(row, 1, 1))
            right = jnp.where(column == width - 1, 0.0, pltpu.roll(row, width - 1, 1))
            for piece in (left, row, right):
                pieces.append(piece.astype(jnp.bfloat16))
        taps = jnp.concatenate(pieces, axis=0)
        row = lax.dot_general(
            taps,
            kin_ref[...],
            (((0,), (0,)), ((), ())),
            preferred_element_type=jnp.float32,
        ).astype(jnp.bfloat16)
        feat[index] = row
        if count:
            add_moments(row)

    def add_moments(row):
        values = row.astype(jnp.float32).reshape(-1, 8, features)
        acc[0] += jnp.sum(values, axis=0)
        acc[1] += jnp.sum(values * values, axis=0)

    def clear_moments():
        acc[...] = jnp.zeros_like(acc)

    def publish(stat, send, recv):
        stat[0] = packed(jnp.sum(acc[...], axis=1))

        def body(d, carry):
            remote(
                stat.at[0], stat.at[d], send.at[d], recv.at[d], lax.rem(me + d, n)
            ).start()
            return carry

        lax.fori_loop(1, n, body, 0)

    def collect(stat, send, recv, gain_ref, bias_ref):
        def body(d, carry):
            remote(
                stat.at[0], stat.at[d], send.at[d], recv.at[d], lax.rem(me + d, n)
            ).wait()
            return carry

        lax.fori_loop(1, n, body, 0)
        row = jnp.sum(stat[...].reshape(n, 128), axis=0, keepdims=True)
        count = n * height * width * (features // GROUPS)
        center, square = [total / count for total in unpacked(row, features)]
        spread = jnp.maximum(square - center * center, 0.0)
        scale = lax.rsqrt(spread + EPSILON) * gain_ref[...]
        return scale, bias_ref[...] - center * scale

    def activate_row(source, index, scale, offset, edge):
        values = source[index].astype(jnp.float32)
        half = (values * scale + offset) * 0.5
        values = half + half * jnp.tanh(half)
        if edge is not None:
            values = jnp.where(edge, values, 0.0)
        stack[index, :, pl.ds(features, features)] = values.astype(jnp.bfloat16)
        stack[index, :, pl.ds(0, features)] = shifted(values, 1).astype(jnp.bfloat16)
        stack[index, :, pl.ds(2 * features, features)] = shifted(values, -1).astype(
            jnp.bfloat16
        )

    def convolve_rows(start, weights):
        total = None
        for a in range(3):
            lhs = stack[pl.ds(start + a, block)].reshape(block * width, 3 * features)
            part = jnp.dot(lhs, weights[a], preferred_element_type=jnp.float32)
            total = part if total is None else total + part
        return total

    lat_up = remote(
        lat.at[pl.ds(2, 2)],
        lat.at[pl.ds(height + 2, 2)],
        lat_send.at[0],
        lat_recv.at[0],
        up,
    )
    lat_down = remote(
        lat.at[pl.ds(height, 2)],
        lat.at[pl.ds(0, 2)],
        lat_send.at[1],
        lat_recv.at[1],
        down,
    )
    for copy in small:
        copy.wait()
    pl.semaphore_wait(barrier, n - 1)

    @pl.when(has_up)
    def _():
        lat_up.start()

    @pl.when(has_down)
    def _():
        lat_down.start()

    clear_moments()

    def inner(index, carry):
        feature_row(index, True)
        return carry

    lax.fori_loop(2, height, inner, 0)

    @pl.when(has_up)
    def _():
        lat_up.wait_send()
        lat_down.wait_recv()

    @pl.when(has_down)
    def _():
        lat_down.wait_send()
        lat_up.wait_recv()

    def edge_row(k, carry):
        feature_row(1 + k * (height - 1), True)
        return carry

    lax.fori_loop(0, 2, edge_row, 0)
    publish(stat_one, one_send, one_recv)
    fetch_two.start()

    def halo_row(k, carry):
        feature_row(k * (height + 1), False)
        return carry

    lax.fori_loop(0, 2, halo_row, 0)
    clear_moments()
    scale, offset = collect(stat_one, one_send, one_recv, gain_one_ref, bias_one_ref)

    def inside(index):
        if index == 0:
            return has_up
        if index == height + 1:
            return has_down
        return None

    def rows_of(number):
        return range(number * block, number * block + block + 2)

    def run_blocks(source, order, scale, offset, ready, emit):
        done = set()

        def fill(indices):
            for index in indices:
                if index not in done:
                    done.add(index)
                    activate_row(source, index, scale, offset, inside(index))

        ready()
        fill(rows_of(order[0]))
        for step, number in enumerate(order):
            following = rows_of(order[step + 1]) if step + 1 < len(order) else ()
            new = [index for index in following if index not in done]
            emit(number, lambda: fill(new))

    hid_up = remote(hid.at[1], hid.at[height + 1], hid_send.at[0], hid_recv.at[0], up)
    hid_down = remote(hid.at[height], hid.at[0], hid_send.at[1], hid_recv.at[1], down)

    def hidden_block(number, beside):
        start = number * block
        rows = convolve_rows(start, k1).astype(jnp.bfloat16)
        beside()
        hid[pl.ds(start + 1, block)] = rows.reshape(block, width, features)
        add_moments(rows)
        if start == 0:

            @pl.when(has_up)
            def _():
                hid_up.start()

        if start == height - block:

            @pl.when(has_down)
            def _():
                hid_down.start()

    last = blocks - 1
    run_blocks(
        feat,
        [last] + list(range(last)),
        scale,
        offset,
        fetch_one.wait,
        hidden_block,
    )
    publish(stat_two, two_send, two_recv)
    scale, offset = collect(stat_two, two_send, two_recv, gain_two_ref, bias_two_ref)

    def wait_hidden():
        fetch_two.wait()

        @pl.when(has_up)
        def _():
            hid_up.wait_send()
            hid_down.wait_recv()

        @pl.when(has_down)
        def _():
            hid_down.wait_send()
            hid_up.wait_recv()

    def final_block(number, beside):
        start = number * block
        rows = convolve_rows(start, k2).reshape(block, width, features)
        beside()
        rows = rows + feat[pl.ds(start + 1, block)].astype(jnp.float32)
        result[pl.ds(start, block)] = rows.astype(jnp.bfloat16)

    run_blocks(
        hid,
        list(range(1, blocks)) + [0],
        scale,
        offset,
        wait_hidden,
        final_block,
    )


def local(n, latent, kernel_in, gain_one, bias_one, kernel_one, gain_two, bias_two, kernel_two):
    channels_in, height, width = latent.shape
    features = kernel_in.shape[3]
    block = 2 if height % 2 == 0 else 1
    bf16 = jnp.bfloat16
    vmem = pl.BlockSpec(memory_space=pltpu.VMEM)
    hbm = pl.BlockSpec(memory_space=pl.ANY)
    dma = pltpu.SemaphoreType.DMA
    return pl.pallas_call(
        functools.partial(kernel, n, block),
        out_shape=pltpu.VMEM((height, width, features), bf16),
        in_specs=[hbm] * 8,
        out_specs=vmem,
        scratch_shapes=[
            pltpu.VMEM((9 * channels_in, features), bf16),
            pltpu.VMEM((1, features), jnp.float32),
            pltpu.VMEM((1, features), jnp.float32),
            pltpu.VMEM((1, features), jnp.float32),
            pltpu.VMEM((1, features), jnp.float32),
            pltpu.VMEM((3, 3 * features, features), bf16),
            pltpu.VMEM((3, 3 * features, features), bf16),
            pltpu.VMEM((height + 4, channels_in, width), bf16),
            pltpu.VMEM((height + 2, width, features), bf16),
            pltpu.VMEM((height + 2, width, 3 * features), bf16),
            pltpu.VMEM((height + 2, width, features), bf16),
            pltpu.VMEM((n, 1, 128), jnp.float32),
            pltpu.VMEM((n, 1, 128), jnp.float32),
            pltpu.VMEM((2, 8, features), jnp.float32),
            dma((2,)),
            dma((6,)),
            dma((2,)),
            dma((2,)),
            dma((2,)),
            dma((2,)),
            dma((n,)),
            dma((n,)),
            dma((n,)),
            dma((n,)),
        ],
        compiler_params=pltpu.CompilerParams(
            collective_id=0, has_side_effects=True, vmem_limit_bytes=56 * 1024 * 1024
        ),
        name="resblock",
    )(
        jnp.transpose(latent, (1, 0, 2)),
        kernel_in.reshape(9 * channels_in, features),
        gain_one.reshape(1, -1),
        bias_one.reshape(1, -1),
        gain_two.reshape(1, -1),
        bias_two.reshape(1, -1),
        kernel_one.reshape(3, 3 * features, features),
        kernel_two.reshape(3, 3 * features, features),
    )


def solution(mesh):
    in_specs = (P(None, ("batch", "rows"), None), P(), P(), P(), P(), P(), P(), P())
    out_specs = P(("batch", "rows"), None, None)
    return jax.shard_map(
        functools.partial(local, mesh.shape["rows"]),
        mesh=mesh,
        in_specs=in_specs,
        out_specs=out_specs,
        check_vma=False,
    )
```
